256 devices in a mesh: row: 8 (over y, core), col: 32 (over x, z).
Axes of the slice: x: 4, y: 4, z: 8, core: 2. Of those that a mesh axis runs over, the one named last changes fastest.
Arguments:
- adjacency: int32 [27136, 27136], P('row', 'col'), may hold values from 0 to 3
- degree: int32 [27136], replicated, may hold values from 64 to 511
- cotangent: bfloat16 [27136, 512], P(('row', 'col')), may hold values from -6 to 6
- features: bfloat16 [27136, 512], P('col'), may hold values from -0.029907227 to 0.029907227
- weight: bfloat16 [512, 512], replicated, may hold values from -0.25 to 0.25
Outputs:
- grad_input: bfloat16 [27136, 512], P('col', 'row')
- grad_weight: float32 [512, 512], P('col', 'row')
The draws below stay inside these ranges and needn't reach their ends.
All inputs are finite; a program needn't handle non-finite values.
Results may differ from the reference program's by a relative error of at most 0.0058.
Values may be sent and summed in bfloat16 or wider, within the bound.
No kernel may reach another device: no remote copies, remote signals or barrier semaphores. Data moves between devices by JAX's collectives and lax.ppermute only.
A program may use at most 128 MiB of HBM per device.

```python
import jax
import jax.numpy as jnp
from jax import lax

F = 512
NODES = 27136
N_ROW = 8


def with_ends(array, own_key, least, high):
    longest = array.shape.index(max(array.shape))
    spots = []
    for shift in (0, 1):
        where = [jax.random.randint(jax.random.fold_in(own_key, axis), (), 0, length) for axis, length in enumerate(array.shape)]
        where[longest] = (where[longest] + shift) % array.shape[longest]
        spots.append(tuple(where))
    return array.at[spots[0]].set(least).at[spots[1]].set(high)


def spiked(array, own_key, source, target, parts, factor):
    owner, partner = [(jnp.arange(array.shape[dim]) // (array.shape[dim] // parts)).reshape([-1 if axis == dim else 1 for axis in range(array.ndim)]) for dim in (source, target)]
    chosen = jax.random.permutation(own_key, parts)[partner]
    strong = (owner == chosen) | (owner == (partner + parts // 2) % parts)
    return jnp.where(strong, factor * array, array)


def block_levels(rng, shape, shards, low, largest):
    def one(position, blocks):
        draws = jax.random.uniform(jax.random.fold_in(jax.random.fold_in(rng, 6), position), (blocks,), jnp.float32, low / len(shards), largest / len(shards))
        return jnp.repeat(jnp.exp(draws), shape[position] // blocks).reshape((-1,) + (1,) * (len(shape) - position - 1))

    gain = one(*shards[0])
    for cut in shards[1:]:
        gain = gain * one(*cut)
    return gain


def noise(key, shape, spread, reach, cuts=(), kind=jnp.bfloat16):
    entries = jax.random.normal(key, shape, jnp.float32) * spread
    if len(cuts) > 0:
        entries = block_levels(key, shape, cuts, -0.22, 0.18) * entries
    return jnp.clip(entries, min=-reach, max=reach).astype(kind)


def bell_draw_with(rng, shape, deviation, most, cuts, heavy, kind=jnp.bfloat16):
    drawn = deviation * jax.random.normal(rng, shape, jnp.float32)
    if cuts:
        drawn = drawn * block_levels(rng, shape, cuts, -0.22, 0.18)
    return jnp.clip(spiked(drawn, jax.random.fold_in(rng, 3), *heavy), -most, most).astype(kind)


def setup_inputs(seed: int = 0) -> dict:
    streams_of = jax.random.split(jax.random.key(seed), 6)
    adjacency = with_ends(jax.random.randint(streams_of[0], (NODES, NODES), 0, 4), jax.random.fold_in(streams_of[0], 1), 0, 3).astype(jnp.int32)
    degree = with_ends(jax.random.randint(streams_of[1], (NODES,), 64, 512), jax.random.fold_in(streams_of[1], 1), 64, 511).astype(jnp.int32)
    cotangent = noise(streams_of[2], (NODES, F), 1.0, 6.0, ((0, 256),))
    features = bell_draw_with(streams_of[3], (NODES, F), 0.005, 0.029907227, ((0, 32),), (0, 1, 32, 2.75))
    weight = noise(streams_of[4], (F, F), F ** -0.5, 0.25)
    return dict(adjacency=adjacency, degree=degree, cotangent=cotangent, features=features, weight=weight)


def reference(adjacency, degree, cotangent, features, weight):
    inv_root = lax.rsqrt(degree.astype(jnp.float32))
    scaled = (cotangent.astype(jnp.float32) * inv_root[:, None]).astype(jnp.bfloat16)
    scaled = lax.optimization_barrier(scaled).astype(jnp.float32)
    step_rows = NODES // N_ROW

    def accumulate(total, index):
        start = (index * step_rows).astype(jnp.int32)
        tile = lax.dynamic_slice_in_dim(adjacency, start, step_rows, 0).astype(jnp.float32)
        block = lax.dynamic_slice_in_dim(scaled, start, step_rows, 0)
        term = jnp.dot(tile.T, block, precision=lax.Precision.HIGHEST, preferred_element_type=jnp.float32)
        return (total + term, None)
    total, _ = lax.scan(accumulate, jnp.zeros((NODES, F), jnp.float32), jnp.arange(N_ROW, dtype=jnp.int32))
    grad_z = (total * inv_root[:, None]).astype(jnp.bfloat16)
    grad_input = jnp.dot(grad_z, weight.T, preferred_element_type=jnp.float32).astype(jnp.bfloat16)
    grad_weight = jnp.dot(features.T, grad_z, preferred_element_type=jnp.float32)
    return (grad_input, grad_weight)
```

```python
import functools

import jax
import jax.numpy as jnp
from jax import lax
from jax.experimental import pallas as pl
from jax.experimental.pallas import tpu as pltpu
from jax.sharding import Mesh
from jax.sharding import PartitionSpec as P


X, Z = "col_0", "col_1"
COL = (X, Z)
ROW_COL = ("row", X, Z)
NT = (((1,), (1,)), ((), ()))
TN = (((0,), (0,)), ((), ()))
CORES = 2

VMEM = pl.BlockSpec(memory_space=pltpu.VMEM)
SMEM = pl.BlockSpec(memory_space=pltpu.SMEM)


def shifted(value, axis, step):
    n = lax.axis_size(axis)
    return lax.ppermute(value, axis, [(i, (i + step) % n) for i in range(n)])


def call(body, out, args, scratch=(), smem=1, flops=1 << 20, limit=16):
    return pl.pallas_call(
        body,
        out_shape=out,
        in_specs=[SMEM] * smem + [VMEM] * (len(args) - smem),
        out_specs=jax.tree.map(lambda _: VMEM, out),
        scratch_shapes=list(scratch),
        compiler_params=pltpu.CompilerParams(vmem_limit_bytes=limit << 20),
        cost_estimate=pl.CostEstimate(flops=flops, bytes_accessed=1 << 20, transcendentals=0),
    )(*args)


def arrange_kernel(steps, me_ref, *refs):
    *pieces, out_ref = refs
    n = out_ref.shape[0]
    for step, ref in zip(steps, pieces):
        out_ref[lax.rem(me_ref[0] + (step + n), n)] = ref[...]


def convert_kernel(tile_ref, out_ref):
    out_ref[...] = tile_ref[...].astype(jnp.float32).astype(jnp.bfloat16)


def product(x_major, me_ref, tile_ref, scale_ref, refs, slots, rows):
    n, m, length, _ = slots.shape
    me = me_ref[0]
    own, _, _ = refs[:3]
    slots[me] = own[...]
    for step in range(1, n // 2):
        up, down = refs[2 * step - 1], refs[2 * step]
        slots[lax.rem(me + (n - step), n)] = up[...]
        slots[lax.rem(me + step, n)] = down[...]
    across = lax.rem(me + n // 2, n)
    slots[across, : m // 2] = refs[-2][...]
    slots[across, m // 2 :] = refs[-1][...]
    for i in range(n):
        for j in range(m):
            k = i * m + j if x_major else j * n + i
            rows[pl.ds(k * length, length), :] = slots[i, j].astype(jnp.float32)
    total = jnp.dot(
        tile_ref[...], rows[...].astype(jnp.bfloat16), preferred_element_type=jnp.float32
    )
    return (total * scale_ref[...]).astype(jnp.bfloat16)


def first_kernel(me_ref, tile_ref, scale_ref, features_ref, *rest):
    *refs, out_ref, r_ref, slots, rows = rest
    out_ref[...] = product(False, me_ref, tile_ref, scale_ref, refs, slots, rows)
    r_ref[...] = lax.dot_general(
        out_ref[...], features_ref[...], TN, preferred_element_type=jnp.float32
    )


def parted(core, held, keep_ref, send_ref):
    for y in range(keep_ref.shape[0]):
        keep_ref[y] = held[CORES * y + core]
        send_ref[y] = held[CORES * y + (CORES - 1 - core)].astype(send_ref.dtype)


def second_kernel(me_ref, tile_ref, scale_ref, features_ref, r_first_ref, *rest):
    *refs, out_ref, keep_ref, send_ref, slots, rows, held = rest
    out_ref[...] = product(True, me_ref, tile_ref, scale_ref, refs, slots, rows)
    r = lax.dot_general(
        out_ref[...], features_ref[...], TN, preferred_element_type=jnp.float32
    )
    n_row, share, width = held.shape
    held[: n_row // 2] = r_first_ref[...].reshape(n_row // 2, share, width)
    held[n_row // 2 :] = r.reshape(n_row // 2, share, width)
    parted(me_ref[1], held, keep_ref, send_ref)


def q_kernel(me_ref, first_ref, second_ref, weight_ref, keep_ref, send_ref, held):
    half = first_ref.shape[1]
    q = lax.dot_general(
        weight_ref[:, :half], first_ref[...], NT, preferred_element_type=jnp.float32
    )
    q += lax.dot_general(
        weight_ref[:, half:], second_ref[...], NT, preferred_element_type=jnp.float32
    )
    held[...] = q.reshape(held.shape)
    parted(me_ref[0], held, keep_ref, send_ref)


def join_kernel(me_ref, keep_ref, got_ref, own_ref, *send_refs):
    n, me = keep_ref.shape[0], me_ref[0]
    own_ref[...] = keep_ref[me] + got_ref[me].astype(jnp.float32)
    for step, ref in enumerate(send_refs, 1):
        to = lax.rem(me + step, n)
        ref[...] = (keep_ref[to] + got_ref[to].astype(jnp.float32)).astype(ref.dtype)


def added(own_ref, refs):
    total = own_ref[...]
    for ref in refs:
        total += ref[...].astype(jnp.float32)
    return total


def pack_kernel(own_ref, *rest):
    *refs, out_ref = rest
    total = added(own_ref, refs)
    n_col, lines, _ = out_ref.shape
    share = total.shape[0]
    blocks = total.T.reshape(n_col, 2 * lines, share)
    out_ref[:, :, :share] = blocks[:, :lines]
    out_ref[:, :, share:] = blocks[:, lines:]


def unpack_kernel(pieces_ref, out_ref):
    lines, share = pieces_ref.shape[1], out_ref.shape[1]
    total = pieces_ref[...].sum(axis=0)
    out_ref[:lines, :] = total[:, :share]
    out_ref[lines:, :] = total[:, share:]


def sum_kernel(own_ref, *rest):
    *refs, out_ref = rest
    out_ref[...] = added(own_ref, refs).astype(out_ref.dtype)


def over_rows(me, keep, send, n_y):
    _, share, length = keep.shape
    n = n_y * CORES
    got = lax.ppermute(send, "row", [(i, i ^ 1) for i in range(n)])
    block = functools.partial(jax.ShapeDtypeStruct, (share, length))
    own, *parts = call(
        join_kernel, (block(jnp.float32),) + (block(jnp.bfloat16),) * (n_y - 1), (me, keep, got)
    )
    arrived = [
        lax.ppermute(part, "row", [(i, (i + CORES * step) % n) for i in range(n)])
        for step, part in enumerate(parts, 1)
    ]
    return own, arrived


def per_device(adjacency, degree, cotangent, features, weight):
    rows_here, cols_here = adjacency.shape
    length, width = cotangent.shape
    half = width // 2
    row = lax.axis_index("row")
    x, z = lax.axis_index(X), lax.axis_index(Z)
    nx, nz = lax.axis_size(X), lax.axis_size(Z)
    n_row = lax.axis_size("row")
    n_y = n_row // CORES
    col = lax.axis_index(COL)
    y, core = row // CORES, row % CORES

    def inv_root(start, size):
        return lax.rsqrt(lax.dynamic_slice_in_dim(degree, start, size, 0).astype(jnp.float32))

    scaled = (
        cotangent.astype(jnp.float32)
        * inv_root(row * rows_here + col * length, length)[:, None]
    ).astype(jnp.bfloat16)
    mine_a, mine_b = scaled[:, :half], scaled[:, half:]
    tile = call(
        convert_kernel,
        jax.ShapeDtypeStruct((cols_here, rows_here), jnp.bfloat16),
        (adjacency.T,),
        smem=0,
        limit=40,
    )
    col_scale = inv_root(col * cols_here, cols_here)[:, None]

    unit = functools.partial(jax.ShapeDtypeStruct, dtype=jnp.bfloat16)
    near = [shifted(mine_a, X, s) for s in range(1, nx)]
    a = call(
        functools.partial(arrange_kernel, [0] + [-s for s in range(1, nx)]),
        unit((nx, length, half)),
        (x.reshape(1), mine_a, *near),
    )
    far = [shifted(mine_b, Z, s) for s in range(1, nz)]
    b = call(
        functools.partial(arrange_kernel, [0] + [-s for s in range(1, nz)]),
        unit((nz, length, half)),
        (z.reshape(1), mine_b, *far),
    )

    def ring(own, axis):
        n = lax.axis_size(axis)
        middle = own.shape[0] // 2
        units, up, down = [own], own, own
        for step in range(1, n // 2 + 1):
            if step == n // 2:
                up, down = up[:middle], down[middle:]
            up = shifted(up, axis, 1)
            down = shifted(down, axis, -1)
            units += [up, down]
        return units

    a_units = ring(a, Z)
    b_units = ring(b, X)

    flops = 2 * rows_here * cols_here * half
    rows_buffer = pltpu.VMEM((rows_here, half), jnp.float32)
    first, r_first = call(
        first_kernel,
        (unit((cols_here, half)), jax.ShapeDtypeStruct((half, width), jnp.float32)),
        (z.reshape(1), tile, col_scale, features, *a_units),
        scratch=(pltpu.VMEM((nz, nx, length, half), jnp.bfloat16), rows_buffer),
        flops=flops,
        limit=32,
    )
    share = width // n_row
    second, r_keep, r_send = call(
        second_kernel,
        (
            unit((cols_here, half)),
            jax.ShapeDtypeStruct((n_y, share, width), jnp.float32),
            unit((n_y, share, width)),
        ),
        (jnp.stack([x, core]), tile, col_scale, features, r_first, *b_units),
        scratch=(
            pltpu.VMEM((nx, nz, length, half), jnp.bfloat16),
            rows_buffer,
            pltpu.VMEM((n_row, share, width), jnp.float32),
        ),
        flops=flops,
        limit=32,
    )
    q_keep, q_send = call(
        q_kernel,
        (
            jax.ShapeDtypeStruct((n_y, share, cols_here), jnp.float32),
            unit((n_y, share, cols_here)),
        ),
        (core.reshape(1), first, second, weight),
        scratch=(pltpu.VMEM((n_row, share, cols_here), jnp.float32),),
        flops=2 * cols_here * width * width,
    )
    r_own, r_parts = over_rows(y.reshape(1), r_keep, r_send, n_y)
    q_own, q_parts = over_rows(y.reshape(1), q_keep, q_send, n_y)

    n_col = nx * nz
    lines = width // n_col // 2
    packed = call(
        pack_kernel,
        jax.ShapeDtypeStruct((n_col, lines, 2 * share), jnp.float32),
        (r_own, *r_parts),
        smem=0,
    )
    w_pieces = lax.all_to_all(packed, COL, split_axis=0, concat_axis=0, tiled=True)
    grad_weight = call(
        unpack_kernel, jax.ShapeDtypeStruct((2 * lines, share), jnp.float32), (w_pieces,), smem=0
    )
    grad_input = call(sum_kernel, unit((share, cols_here)), (q_own, *q_parts), smem=0).T
    return (grad_input, grad_weight)


def solution(mesh):
    torus = Mesh(mesh.devices.reshape(mesh.shape["row"], 4, 8), ("row", X, Z))
    placed = (P("row", COL), P(), P(ROW_COL, None), P(COL, None), P())
    return jax.shard_map(
        per_device,
        mesh=torus,
        in_specs=placed,
        out_specs=(P(COL, "row"), P(COL, "row")),
        check_vma=False,
    )
```

```python
import functools

import jax
import jax.numpy as jnp
from jax import lax
from jax.experimental import pallas as pl
from jax.experimental.pallas import tpu as pltpu
from jax.sharding import Mesh
from jax.sharding import PartitionSpec as P


X, Z = "col_0", "col_1"
COL = (X, Z)
ROW_COL = ("row", X, Z)
NT = (((1,), (1,)), ((), ()))
TN = (((0,), (0,)), ((), ()))
CORES = 2
LANES = 128

VMEM = pl.BlockSpec(memory_space=pltpu.VMEM)
SMEM = pl.BlockSpec(memory_space=pltpu.SMEM)


def shifted(value, axis, step):
    n = lax.axis_size(axis)
    return lax.ppermute(value, axis, [(i, (i + step) % n) for i in range(n)])


def call(body, out, args, scratch=(), smem=1, flops=1 << 20, limit=16, aliases=()):
    return pl.pallas_call(
        body,
        out_shape=out,
        in_specs=[SMEM] * smem + [VMEM] * (len(args) - smem),
        out_specs=jax.tree.map(lambda _: VMEM, out),
        scratch_shapes=list(scratch),
        input_output_aliases=dict(aliases),
        compiler_params=pltpu.CompilerParams(vmem_limit_bytes=limit << 20),
        cost_estimate=pl.CostEstimate(flops=flops, bytes_accessed=1 << 20, transcendentals=0),
    )(*args)


def arrange_kernel(me_ref, *refs):
    *pieces, out_0, out_1 = refs
    n, (length, half) = len(pieces), (pieces[0].shape[0], out_0.shape[1])
    for me in range(n):

        @pl.when(me_ref[0] == me)
        def _():
            for step, ref in enumerate(pieces):
                here = pl.ds((me - step) % n * length, length)
                out_0[here, :] = ref[:, :half]
                out_1[here, :] = ref[:, half:]


def cut_kernel(start, value_ref, out_ref):
    out_ref[...] = value_ref[pl.ds(start, out_ref.shape[0]), :]


def convert_kernel(start, tile_hbm, out_ref, held, sems):
    step = 16
    parts = sems.shape[0]
    groups = held.shape[0] // step
    bounds = [groups * k // parts for k in range(parts + 1)]

    def copy(k):
        here, size = bounds[k] * step, (bounds[k + 1] - bounds[k]) * step
        return pltpu.make_async_copy(
            tile_hbm.at[pl.ds(start + here, size), :], held.at[pl.ds(here, size), :], sems.at[k]
        )

    for k in range(parts):
        copy(k).start()
    for k in range(parts):
        copy(k).wait()

        @pl.loop(bounds[k], bounds[k + 1])
        def _(i):
            here = pl.ds(pl.multiple_of(i * step, step), step)
            out_ref[here, :] = held[here, :].astype(jnp.float32).astype(jnp.bfloat16)


def lay(me, n_x, n_z, units, rows_refs):
    for step, parts in units:
        z = lax.rem(me + (n_z + step), n_z)
        length = sum(ref.shape[0] for ref in parts) // n_x
        first = 0
        for ref in parts:
            last = first + ref.shape[0]
            for x in range(n_x):
                a, b = max(first, x * length), min(last, (x + 1) * length)
                if a < b:
                    here = pl.ds((x * n_z + z) * length + (a - x * length), b - a)
                    for c, rows_ref in enumerate(rows_refs):
                        rows_ref[here, :] = ref[
                            a - first : b - first, c * LANES : (c + 1) * LANES
                        ].astype(jnp.float32)
            first = last


def early_kernel(n_x, n_z, me_ref, *rest):
    *units, rows_0, rows_1 = rest
    steps = [0] + [s * k for k in range(1, n_z // 2) for s in (-1, 1)]
    lay(me_ref[0], n_x, n_z, [(s, [ref]) for s, ref in zip(steps, units)], (rows_0, rows_1))


def late(n_x, n_z, me, tile_refs, scale_ref, up, down, rows_refs, out_ref):
    lay(me, n_x, n_z, [(n_z // 2, [up, down])], rows_refs)
    rows = jnp.concatenate([ref[...].astype(jnp.bfloat16) for ref in rows_refs], axis=1)
    first = 0
    for tile_ref in tile_refs:
        here = pl.ds(first, tile_ref.shape[0])
        total = jnp.dot(tile_ref[...], rows, preferred_element_type=jnp.float32)
        out_ref[here, :] = (total * scale_ref[here, :]).astype(jnp.bfloat16)
        first += tile_ref.shape[0]


def first_kernel(n_x, n_z, me_ref, tile_0, tile_1, scale_ref, features_ref, *rest):
    up, down, _, _, out_ref, r_ref, *rows_refs = rest
    late(n_x, n_z, me_ref[0], (tile_0, tile_1), scale_ref, up, down, rows_refs, out_ref)
    r_ref[...] = lax.dot_general(
        out_ref[...], features_ref[...], TN, preferred_element_type=jnp.float32
    )


def parted(core, held, keep_ref, send_ref):
    for y in range(keep_ref.shape[0]):
        keep_ref[y] = held[CORES * y + core]
        send_ref[y] = held[CORES * y + (CORES - 1 - core)].astype(send_ref.dtype)


def second_kernel(
    n_x, n_z, me_ref, core_ref, tile_0, tile_1, scale_ref, features_ref, r_first_ref, *rest
):
    up, down, _, _, out_ref, keep_ref, send_ref, *rows_refs, held = rest
    late(n_x, n_z, me_ref[0], (tile_0, tile_1), scale_ref, up, down, rows_refs, out_ref)
    r = lax.dot_general(
        out_ref[...], features_ref[...], TN, preferred_element_type=jnp.float32
    )
    n_row, share, width = held.shape
    held[: n_row // 2] = r_first_ref[...].reshape(n_row // 2, share, width)
    held[n_row // 2 :] = r.reshape(n_row // 2, share, width)
    parted(core_ref[0], held, keep_ref, send_ref)


def q_kernel(me_ref, first_ref, second_ref, weight_ref, keep_ref, send_ref, held):
    half = first_ref.shape[1]
    q = lax.dot_general(
        weight_ref[:, :half], first_ref[...], NT, preferred_element_type=jnp.float32
    )
    q += lax.dot_general(
        weight_ref[:, half:], second_ref[...], NT, preferred_element_type=jnp.float32
    )
    held[...] = q.reshape(held.shape)
    parted(me_ref[0], held, keep_ref, send_ref)


def join_kernel(me_ref, keep_ref, got_ref, own_ref, *send_refs):
    n, me = keep_ref.shape[0], me_ref[0]
    own_ref[...] = keep_ref[me] + got_ref[me].astype(jnp.float32)
    for step, ref in enumerate(send_refs, 1):
        to = lax.rem(me + step, n)
        ref[...] = (keep_ref[to] + got_ref[to].astype(jnp.float32)).astype(ref.dtype)


def added(own_ref, refs):
    total = own_ref[...]
    for ref in refs:
        total += ref[...].astype(jnp.float32)
    return total


def pack_kernel(own_ref, *rest):
    *refs, out_ref = rest
    total = added(own_ref, refs)
    n_col, lines, _ = out_ref.shape
    share = total.shape[0]
    blocks = total.T.reshape(n_col, 2 * lines, share)
    out_ref[:, :, :share] = blocks[:, :lines]
    out_ref[:, :, share:] = blocks[:, lines:]


def unpack_kernel(pieces_ref, out_ref):
    lines, share = pieces_ref.shape[1], out_ref.shape[1]
    total = pieces_ref[...].sum(axis=0)
    out_ref[:lines, :] = total[:, :share]
    out_ref[lines:, :] = total[:, share:]


def sum_kernel(own_ref, *rest):
    *refs, out_ref = rest
    out_ref[...] = added(own_ref, refs).astype(out_ref.dtype)


def over_rows(me, keep, send, n_y):
    _, share, length = keep.shape
    n = n_y * CORES
    got = lax.ppermute(send, "row", [(i, i ^ 1) for i in range(n)])
    block = functools.partial(jax.ShapeDtypeStruct, (share, length))
    own, *parts = call(
        join_kernel, (block(jnp.float32),) + (block(jnp.bfloat16),) * (n_y - 1), (me, keep, got)
    )
    arrived = [
        lax.ppermute(part, "row", [(i, (i + CORES * step) % n) for i in range(n)])
        for step, part in enumerate(parts, 1)
    ]
    return own, arrived


def per_device(adjacency, degree, cotangent, features, weight):
    rows_here, cols_here = adjacency.shape
    length, width = cotangent.shape
    half = width // 2
    row = lax.axis_index("row")
    x, z = lax.axis_index(X), lax.axis_index(Z)
    nx, nz = lax.axis_size(X), lax.axis_size(Z)
    n_row = lax.axis_size("row")
    n_y = n_row // CORES
    col = lax.axis_index(COL)
    y, core = lax.div(row, CORES), lax.rem(row, CORES)

    row_start = (row * rows_here + col * length).astype(jnp.uint32)
    col_start = (col * cols_here).astype(jnp.uint32)
    cotangent, x, z, y, core, row_start, col_start = lax.optimization_barrier(
        (cotangent, x, z, y, core, row_start, col_start)
    )

    def inv_root(start, size):
        return lax.rsqrt(lax.dynamic_slice(degree, (start,), (size,)).astype(jnp.float32))

    scaled = (
        cotangent.astype(jnp.float32)
        * inv_root(row_start, length)[:, None]
    ).astype(jnp.bfloat16)
    col_scale = inv_root(col_start, cols_here)[:, None]

    def converted(start, size):
        return pl.pallas_call(
            functools.partial(convert_kernel, start),
            out_shape=jax.ShapeDtypeStruct((size, rows_here), jnp.bfloat16),
            in_specs=[pl.BlockSpec(memory_space=pltpu.HBM)],
            out_specs=VMEM,
            scratch_shapes=[
                pltpu.VMEM((size, rows_here), jnp.int32),
                pltpu.SemaphoreType.DMA((4,)),
            ],
            compiler_params=pltpu.CompilerParams(vmem_limit_bytes=46 << 20),
            cost_estimate=pl.CostEstimate(flops=1 << 24, bytes_accessed=9 << 20, transcendentals=0),
            name="convert",
        )(adjacency.T)

    split = cols_here // 32 * 16
    tiles = (converted(0, split), converted(split, cols_here - split))

    unit = functools.partial(jax.ShapeDtypeStruct, dtype=jnp.bfloat16)

    near = [shifted(scaled, X, s) for s in range(1, nx)]
    run = nx * length
    middle = run // 2 // 16 * 16
    a, b = call(
        arrange_kernel, (unit((run, half)), unit((run, half))), (x.reshape(1), scaled, *near)
    )

    def cut(value, start, stop):
        return call(
            functools.partial(cut_kernel, start), unit((stop - start, half)), (value,), smem=0
        )

    def ring(own):
        units, up, down = [own], own, own
        for step in range(1, nz // 2 + 1):
            if step == nz // 2:
                up, down = cut(up, 0, middle), cut(down, middle, run)
            up = shifted(up, Z, 1)
            down = shifted(down, Z, -1)
            units += [up, down]
        return units

    column = jax.ShapeDtypeStruct((rows_here, LANES), jnp.float32)

    def early(units):
        return call(
            functools.partial(early_kernel, nx, nz), (column, column), (z.reshape(1), *units)
        )

    flops = 2 * rows_here * cols_here * half
    a_units, b_units = ring(a), ring(b)
    first, r_first, *_ = call(
        functools.partial(first_kernel, nx, nz),
        (unit((cols_here, half)), jax.ShapeDtypeStruct((half, width), jnp.float32), column, column),
        (z.reshape(1), *tiles, col_scale, features, *a_units[7:], *early(a_units[:7])),
        flops=flops,
        aliases={7: 2, 8: 3},
    )
    share = width // n_row
    second, r_keep, r_send, *_ = call(
        functools.partial(second_kernel, nx, nz),
        (
            unit((cols_here, half)),
            jax.ShapeDtypeStruct((n_y, share, width), jnp.float32),
            unit((n_y, share, width)),
            column,
            column,
        ),
        (
            z.reshape(1),
            core.reshape(1),
            *tiles,
            col_scale,
            features,
            r_first,
            *b_units[7:],
            *early(b_units[:7]),
        ),
        scratch=(pltpu.VMEM((n_row, share, width), jnp.float32),),
        smem=2,
        flops=flops,
        aliases={9: 3, 10: 4},
    )
    q_keep, q_send = call(
        q_kernel,
        (
            jax.ShapeDtypeStruct((n_y, share, cols_here), jnp.float32),
            unit((n_y, share, cols_here)),
        ),
        (core.reshape(1), first, second, weight),
        scratch=(pltpu.VMEM((n_row, share, cols_here), jnp.float32),),
        flops=2 * cols_here * width * width,
    )
    r_own, r_parts = over_rows(y.reshape(1), r_keep, r_send, n_y)
    q_own, q_parts = over_rows(y.reshape(1), q_keep, q_send, n_y)

    n_col = nx * nz
    lines = width // n_col // 2
    packed = call(
        pack_kernel,
        jax.ShapeDtypeStruct((n_col, lines, 2 * share), jnp.float32),
        (r_own, *r_parts),
        smem=0,
    )
    w_pieces = lax.all_to_all(packed, COL, split_axis=0, concat_axis=0, tiled=True)
    grad_weight = call(
        unpack_kernel, jax.ShapeDtypeStruct((2 * lines, share), jnp.float32), (w_pieces,), smem=0
    )
    grad_input = call(sum_kernel, unit((share, cols_here)), (q_own, *q_parts), smem=0).T
    return (grad_input, grad_weight)


def solution(mesh):
    torus = Mesh(mesh.devices.reshape(mesh.shape["row"], 4, 8), ("row", X, Z))
    placed = (P("row", COL), P(), P(ROW_COL, None), P(COL, None), P())
    return jax.shard_map(
        per_device,
        mesh=torus,
        in_specs=placed,
        out_specs=(P(COL, "row"), P(COL, "row")),
        check_vma=False,
    )
```

```python
import functools

import jax
import jax.numpy as jnp
from jax import lax
from jax.experimental import pallas as pl
from jax.experimental.pallas import tpu as pltpu
from jax.sharding import Mesh
from jax.sharding import PartitionSpec as P


X, Z = "col_0", "col_1"
COL = (X, Z)
ROW_COL = ("row", X, Z)
NT = (((1,), (1,)), ((), ()))
TN = (((0,), (0,)), ((), ()))
CORES = 2
LANES = 128

VMEM = pl.BlockSpec(memory_space=pltpu.VMEM)
SMEM = pl.BlockSpec(memory_space=pltpu.SMEM)


def shifted(value, axis, step):
    n = lax.axis_size(axis)
    return lax.ppermute(value, axis, [(i, (i + step) % n) for i in range(n)])


def call(body, out, args, scratch=(), smem=1, flops=1 << 20, limit=16, aliases=()):
    return pl.pallas_call(
        body,
        out_shape=out,
        in_specs=[SMEM] * smem + [VMEM] * (len(args) - smem),
        out_specs=jax.tree.map(lambda _: VMEM, out),
        scratch_shapes=list(scratch),
        input_output_aliases=dict(aliases),
        compiler_params=pltpu.CompilerParams(vmem_limit_bytes=limit << 20),
        cost_estimate=pl.CostEstimate(flops=flops, bytes_accessed=1 << 20, transcendentals=0),
    )(*args)


def arrange_kernel(me_ref, *refs):
    *pieces, out_0, out_1 = refs
    n, (length, half) = len(pieces), (pieces[0].shape[0], out_0.shape[1])
    for me in range(n):

        @pl.when(me_ref[0] == me)
        def _():
            for step, ref in enumerate(pieces):
                here = pl.ds((me - step) % n * length, length)
                out_0[here, :] = ref[:, :half]
                out_1[here, :] = ref[:, half:]


def cut_kernel(start, value_ref, out_ref):
    out_ref[...] = value_ref[pl.ds(start, out_ref.shape[0]), :]


def convert_kernel(start, tile_hbm, out_ref, held, sems):
    step = 16
    parts = sems.shape[0]
    groups = held.shape[0] // step
    bounds = [groups * k // parts for k in range(parts + 1)]

    def copy(k):
        here, size = bounds[k] * step, (bounds[k + 1] - bounds[k]) * step
        return pltpu.make_async_copy(
            tile_hbm.at[pl.ds(start + here, size), :], held.at[pl.ds(here, size), :], sems.at[k]
        )

    for k in range(parts):
        copy(k).start()
    for k in range(parts):
        copy(k).wait()

        @pl.loop(bounds[k], bounds[k + 1])
        def _(i):
            here = pl.ds(pl.multiple_of(i * step, step), step)
            out_ref[here, :] = held[here, :].astype(jnp.float32).astype(jnp.bfloat16)


def lay(me, n_x, n_z, units, rows_refs):
    for step, parts in units:
        z = lax.rem(me + (n_z + step), n_z)
        length = sum(ref.shape[0] for ref in parts) // n_x
        first = 0
        for ref in parts:
            last = first + ref.shape[0]
            for x in range(n_x):
                a, b = max(first, x * length), min(last, (x + 1) * length)
                if a < b:
                    here = pl.ds((x * n_z + z) * length + (a - x * length), b - a)
                    for c, rows_ref in enumerate(rows_refs):
                        rows_ref[here, :] = ref[
                            a - first : b - first, c * LANES : (c + 1) * LANES
                        ].astype(jnp.float32)
            first = last


def early_kernel(n_x, n_z, me_ref, *rest):
    *units, rows_0, rows_1 = rest
    steps = [0] + [s * k for k in range(1, n_z // 2) for s in (-1, 1)]
    lay(me_ref[0], n_x, n_z, [(s, [ref]) for s, ref in zip(steps, units)], (rows_0, rows_1))


def late(n_x, n_z, me, tile_refs, scale_ref, up, down, rows_refs, out_ref):
    lay(me, n_x, n_z, [(n_z // 2, [up, down])], rows_refs)
    rows = jnp.concatenate([ref[...].astype(jnp.bfloat16) for ref in rows_refs], axis=1)
    first = 0
    for tile_ref in tile_refs:
        here = pl.ds(first, tile_ref.shape[0])
        total = jnp.dot(tile_ref[...], rows, preferred_element_type=jnp.float32)
        out_ref[here, :] = (total * scale_ref[here, :]).astype(jnp.bfloat16)
        first += tile_ref.shape[0]


def first_kernel(n_x, n_z, me_ref, tile_0, tile_1, scale_ref, features_ref, *rest):
    up, down, _, _, out_ref, r_ref, *rows_refs = rest
    late(n_x, n_z, me_ref[0], (tile_0, tile_1), scale_ref, up, down, rows_refs, out_ref)
    r_ref[...] = lax.dot_general(
        out_ref[...], features_ref[...], TN, preferred_element_type=jnp.float32
    )


def parted(core, held, keep_ref, send_ref):
    for y in range(keep_ref.shape[0]):
        keep_ref[y] = held[CORES * y + core]
        send_ref[y] = held[CORES * y + (CORES - 1 - core)].astype(send_ref.dtype)


def second_kernel(
    n_x, n_z, me_ref, core_ref, tile_0, tile_1, scale_ref, features_ref, r_first_ref, *rest
):
    up, down, _, _, out_ref, keep_ref, send_ref, *rows_refs, held = rest
    late(n_x, n_z, me_ref[0], (tile_0, tile_1), scale_ref, up, down, rows_refs, out_ref)
    r = lax.dot_general(
        out_ref[...], features_ref[...], TN, preferred_element_type=jnp.float32
    )
    n_row, share, width = held.shape
    held[: n_row // 2] = r_first_ref[...].reshape(n_row // 2, share, width)
    held[n_row // 2 :] = r.reshape(n_row // 2, share, width)
    parted(core_ref[0], held, keep_ref, send_ref)


def q_kernel(me_ref, first_ref, second_ref, weight_ref, keep_ref, send_ref, held):
    half = first_ref.shape[1]
    q = lax.dot_general(
        weight_ref[:, :half], first_ref[...], NT, preferred_element_type=jnp.float32
    )
    q += lax.dot_general(
        weight_ref[:, half:], second_ref[...], NT, preferred_element_type=jnp.float32
    )
    held[...] = q.reshape(held.shape)
    parted(me_ref[0], held, keep_ref, send_ref)


def join_kernel(me_ref, keep_ref, got_ref, own_ref, *send_refs):
    n, me = keep_ref.shape[0], me_ref[0]
    own_ref[...] = keep_ref[me] + got_ref[me].astype(jnp.float32)
    for step, ref in enumerate(send_refs, 1):
        to = lax.rem(me + step, n)
        ref[...] = (keep_ref[to] + got_ref[to].astype(jnp.float32)).astype(ref.dtype)


def added(own_ref, refs):
    total = own_ref[...]
    for ref in refs:
        total += ref[...].astype(jnp.float32)
    return total


def pack_kernel(own_ref, *rest):
    *refs, out_ref = rest
    total = added(own_ref, refs)
    n_col, lines, _ = out_ref.shape
    share = total.shape[0]
    blocks = total.T.reshape(n_col, 2 * lines, share)
    out_ref[:, :, :share] = blocks[:, :lines]
    out_ref[:, :, share:] = blocks[:, lines:]


def last_kernel(pieces_ref, own_ref, *rest):
    *refs, weight_ref, input_ref = rest
    input_ref[...] = added(own_ref, refs).astype(input_ref.dtype)
    lines, share = pieces_ref.shape[1], weight_ref.shape[1]
    total = pieces_ref[...].sum(axis=0)
    weight_ref[:lines, :] = total[:, :share]
    weight_ref[lines:, :] = total[:, share:]


def over_rows(me, keep, send, n_y):
    _, share, length = keep.shape
    n = n_y * CORES
    got = lax.ppermute(send, "row", [(i, i ^ 1) for i in range(n)])
    block = functools.partial(jax.ShapeDtypeStruct, (share, length))
    own, *parts = call(
        join_kernel, (block(jnp.float32),) + (block(jnp.bfloat16),) * (n_y - 1), (me, keep, got)
    )
    arrived = [
        lax.ppermute(part, "row", [(i, (i + CORES * step) % n) for i in range(n)])
        for step, part in enumerate(parts, 1)
    ]
    return own, arrived


def per_device(adjacency, degree, cotangent, features, weight):
    rows_here, cols_here = adjacency.shape
    length, width = cotangent.shape
    half = width // 2
    row = lax.axis_index("row")
    x, z = lax.axis_index(X), lax.axis_index(Z)
    nx, nz = lax.axis_size(X), lax.axis_size(Z)
    n_row = lax.axis_size("row")
    n_y = n_row // CORES
    col = lax.axis_index(COL)
    y, core = lax.div(row, CORES), lax.rem(row, CORES)

    row_start = (row * rows_here + col * length).astype(jnp.uint32)
    col_start = (col * cols_here).astype(jnp.uint32)
    cotangent, x, z, y, core, row_start, col_start = lax.optimization_barrier(
        (cotangent, x, z, y, core, row_start, col_start)
    )

    def inv_root(start, size):
        return lax.rsqrt(lax.dynamic_slice(degree, (start,), (size,)).astype(jnp.float32))

    scaled = (
        cotangent.astype(jnp.float32)
        * inv_root(row_start, length)[:, None]
    ).astype(jnp.bfloat16)
    col_scale = inv_root(col_start, cols_here)[:, None]

    def converted(start, size):
        return pl.pallas_call(
            functools.partial(convert_kernel, start),
            out_shape=jax.ShapeDtypeStruct((size, rows_here), jnp.bfloat16),
            in_specs=[pl.BlockSpec(memory_space=pltpu.HBM)],
            out_specs=VMEM,
            scratch_shapes=[
                pltpu.VMEM((size, rows_here), jnp.int32),
                pltpu.SemaphoreType.DMA((4,)),
            ],
            compiler_params=pltpu.CompilerParams(vmem_limit_bytes=46 << 20),
            cost_estimate=pl.CostEstimate(flops=1 << 24, bytes_accessed=9 << 20, transcendentals=0),
            name="convert",
        )(adjacency.T)

    split = cols_here // 32 * 16
    tiles = (converted(0, split), converted(split, cols_here - split))

    unit = functools.partial(jax.ShapeDtypeStruct, dtype=jnp.bfloat16)

    near = [shifted(scaled, X, s) for s in range(1, nx)]
    run = nx * length
    middle = run // 2 // 16 * 16
    a, b = call(
        arrange_kernel, (unit((run, half)), unit((run, half))), (x.reshape(1), scaled, *near)
    )

    def cut(value, start, stop):
        return call(
            functools.partial(cut_kernel, start), unit((stop - start, half)), (value,), smem=0
        )

    def ring(own):
        units, up, down = [own], own, own
        for step in range(1, nz // 2 + 1):
            if step == nz // 2:
                up, down = cut(up, 0, middle), cut(down, middle, run)
            up = shifted(up, Z, 1)
            down = shifted(down, Z, -1)
            units += [up, down]
        return units

    column = jax.ShapeDtypeStruct((rows_here, LANES), jnp.float32)

    def early(units):
        return call(
            functools.partial(early_kernel, nx, nz), (column, column), (z.reshape(1), *units)
        )

    flops = 2 * rows_here * cols_here * half
    a_units, b_units = ring(a), ring(b)
    first, r_first, *_ = call(
        functools.partial(first_kernel, nx, nz),
        (unit((cols_here, half)), jax.ShapeDtypeStruct((half, width), jnp.float32), column, column),
        (z.reshape(1), *tiles, col_scale, features, *a_units[7:], *early(a_units[:7])),
        flops=flops,
        aliases={7: 2, 8: 3},
    )
    share = width // n_row
    second, r_keep, r_send, *_ = call(
        functools.partial(second_kernel, nx, nz),
        (
            unit((cols_here, half)),
            jax.ShapeDtypeStruct((n_y, share, width), jnp.float32),
            unit((n_y, share, width)),
            column,
            column,
        ),
        (
            z.reshape(1),
            core.reshape(1),
            *tiles,
            col_scale,
            features,
            r_first,
            *b_units[7:],
            *early(b_units[:7]),
        ),
        scratch=(pltpu.VMEM((n_row, share, width), jnp.float32),),
        smem=2,
        flops=flops,
        aliases={9: 3, 10: 4},
    )
    q_keep, q_send = call(
        q_kernel,
        (jax.ShapeDtypeStruct((n_y, share, cols_here), jnp.float32), unit((n_y, share, cols_here))),
        (core.reshape(1), first, second, weight),
        scratch=(pltpu.VMEM((n_row, share, cols_here), jnp.float32),),
        flops=2 * cols_here * width * width,
    )
    r_own, r_parts = over_rows(y.reshape(1), r_keep, r_send, n_y)
    q_own, q_parts = over_rows(y.reshape(1), q_keep, q_send, n_y)

    n_col = nx * nz
    lines = width // n_col // 2
    packed = call(
        pack_kernel,
        jax.ShapeDtypeStruct((n_col, lines, 2 * share), jnp.float32),
        (r_own, *r_parts),
        smem=0,
    )
    w_pieces = lax.all_to_all(packed, COL, split_axis=0, concat_axis=0, tiled=True)
    grad_weight, grad_input = call(
        last_kernel,
        (jax.ShapeDtypeStruct((2 * lines, share), jnp.float32), unit((share, cols_here))),
        (w_pieces, q_own, *q_parts),
        smem=0,
    )
    return (grad_input.T, grad_weight)


def solution(mesh):
    torus = Mesh(mesh.devices.reshape(mesh.shape["row"], 4, 8), ("row", X, Z))
    placed = (P("row", COL), P(), P(ROW_COL, None), P(COL, None), P())
    return jax.shard_map(
        per_device,
        mesh=torus,
        in_specs=placed,
        out_specs=(P(COL, "row"), P(COL, "row")),
        check_vma=False,
    )
```
